32 devices in a mesh: section: 4 (over y, x), mp: 8 (over z, core).
Axes of the slice: x: 2, y: 2, z: 4, core: 2. Of those that a mesh axis runs over, the one named last changes fastest.
Arguments:
- hidden_in: bfloat16 [1, 4, 64, 4096], P(None, 'section'), may hold values from -36 to 36
- attn_gain: bfloat16 [4, 4096], P('section'), may hold values from 0.5 to 2
- w_query: bfloat16 [4, 4096, 4096], P('section', None, 'mp'), may hold values from -0.75 to 0.75
- w_key: bfloat16 [4, 4096, 1024], P('section', None, 'mp'), may hold values from -0.0625 to 0.0625
- w_value: bfloat16 [4, 4096, 1024], P('section', None, 'mp'), may hold values from -0.09375 to 0.09375
- w_out: bfloat16 [4, 4096, 4096], P('section', 'mp'), may hold values from -0.09375 to 0.09375
- ffn_gain: bfloat16 [4, 4096], P('section'), may hold values from 0.5 to 2
- w_gate: bfloat16 [4, 4096, 14336], P('section', None, 'mp'), may hold values from -0.09375 to 0.09375
- w_up: bfloat16 [4, 4096, 14336], P('section', None, 'mp'), may hold values from -0.09375 to 0.09375
- w_down: bfloat16 [4, 14336, 4096], P('section', 'mp'), may hold values from -0.046875 to 0.046875
- ffn_blocks: int32 [4, 4], P(None, 'section'), may hold values from 1 to 112
- heads_on: int32 [4, 4], P(None, 'section'), may hold values from 1 to 32
Outputs:
- hidden_out: bfloat16 [1, 4, 64, 4096], P(None, 'section')
The draws below stay inside these ranges and needn't reach their ends.
Inputs may be any that keep to these rules, and one draw needn't show every extreme that they name: `ffn_blocks`: hidden units below 128 times the entry are active. `heads_on`: query heads below the entry are active.
All inputs are finite; a program needn't handle non-finite values.
Results may differ from the reference program's by a relative error of at most 0.025.
Values may be sent and summed in bfloat16 or wider, within the bound.
A program may use at most 128 MiB of HBM per device.

```python
import math
import jax
import jax.numpy as jnp
from jax import lax

D = 4096
HEADS = 32
KV_HEADS = 8
HD = 128
BLOCK = 128
FFB = 112
FF = 14336
FFP = 14336
SECTIONS = 4
LAYERS = 4
LEN = 64
MICRO_DEV = 1
MICRO = 4
N_MP = 8


def query_key_pair(key):
    folded = jax.random.fold_in(key, 7101)
    key_keys, key_query = jax.random.split(folded, 2)
    query_shape = (LAYERS, D, HEADS * HD)
    key_shape = (LAYERS, D, KV_HEADS * HD)
    spread_scale = D ** (-0.5)
    key_weight = jnp.clip(jax.random.normal(key_keys, key_shape, jnp.float32), -4.0, 4.0) * spread_scale
    query_weight = jnp.clip(jax.random.normal(key_query, query_shape, jnp.float32), -4.0, 4.0) * spread_scale
    return (query_weight, key_weight)


def draw_w_query(key, part):
    return query_key_pair(key)[0].astype(jnp.bfloat16)


def draw_w_key(key, part):
    return query_key_pair(key)[1].astype(jnp.bfloat16)


def draw_hidden_in(key, part):
    folded = jax.random.fold_in(key, 7202)
    key_noise, key_rows, key_columns = jax.random.split(folded, 3)
    array_shape = (MICRO_DEV, SECTIONS, LEN, D)
    low_end = jnp.log(0.3)
    high_end = jnp.log(3.0)
    row_scale = jnp.exp(jax.random.uniform(key_rows, (MICRO_DEV, SECTIONS, LEN, 1), jnp.float32, low_end, high_end))
    col_scale = jnp.exp(jax.random.uniform(key_columns, (1, 1, 1, D), jnp.float32, low_end, high_end))
    jitter = jnp.clip(jax.random.normal(key_noise, array_shape, jnp.float32), -4.0, 4.0)
    return (jitter * row_scale * col_scale).astype(jnp.bfloat16)


def place_ends(array, stream_key, least, high):
    index_at = [jax.random.randint(jax.random.fold_in(stream_key, axis), (), 0, length) for axis, length in enumerate(array.shape)]
    longest = array.shape.index(max(array.shape))
    next_to = index_at[:longest] + [(index_at[longest] + 1) % array.shape[longest]] + index_at[longest + 1:]
    return array.at[tuple(index_at)].set(least).at[tuple(next_to)].set(high)


def shard_levels(stream_key, shape, pieces, smallest, top_value):
    factor_of = 1.0
    for dim, shards_of in pieces:
        steps = jax.random.uniform(jax.random.fold_in(jax.random.fold_in(stream_key, 6), dim), (shards_of,), jnp.float32, smallest / len(pieces), top_value / len(pieces))
        factor_of = factor_of * jnp.repeat(jnp.exp(steps), shape[dim] // shards_of).reshape((-1,) + (1,) * (len(shape) - 1 - dim))
    return factor_of


def centred(key, extent, width, reach, pieces=(), held_as=jnp.bfloat16):
    factor_of = shard_levels(key, extent, pieces, -0.22, 0.18) if pieces else 1.0
    values = jax.random.normal(key, extent, jnp.float32) * width * factor_of
    return jnp.minimum(jnp.maximum(values, -reach), reach).astype(held_as)


def setup_inputs(seed: int = 0) -> dict:
    keys = jax.random.split(jax.random.key(seed), 13)
    hidden_in = draw_hidden_in(jax.random.fold_in(keys[12], 71), 0)
    attn_gain = jnp.clip(jnp.exp(math.log(2.0) - 1.3862944 * jax.random.uniform(keys[1], (LAYERS, D), jnp.float32) ** shard_levels(keys[1], (LAYERS, D), ((0, 4),), -0.2, 0.2)), 0.5, 2.0).astype(jnp.bfloat16)
    w_query = draw_w_query(jax.random.fold_in(keys[12], 71), 0)
    w_key = draw_w_key(jax.random.fold_in(keys[12], 71), 0)
    w_value = centred(keys[4], (LAYERS, D, KV_HEADS * HD), D ** -0.5, 0.09375, ((0, 4), (2, 8)))
    w_out = centred(keys[5], (LAYERS, HEADS * HD, D), (HEADS * HD) ** -0.5, 0.09375, ((0, 4), (1, 8)))
    ffn_gain = jnp.clip(jnp.exp(math.log(2.0) - 1.3862944 * jax.random.uniform(keys[6], (LAYERS, D), jnp.float32) ** shard_levels(keys[6], (LAYERS, D), ((0, 4),), -0.2, 0.2)), 0.5, 2.0).astype(jnp.bfloat16)
    w_gate = centred(keys[7], (LAYERS, D, FFP), D ** -0.5, 0.09375, ((0, 4), (2, 8)))
    w_up = centred(keys[8], (LAYERS, D, FFP), D ** -0.5, 0.09375, ((0, 4), (2, 8)))
    w_down = centred(keys[9], (LAYERS, FFP, D), FF ** -0.5, 0.046875, ((0, 4), (1, 8)))
    ffn_blocks = place_ends(jax.random.randint(keys[10], (MICRO, LAYERS), 1, FFB + 1), jax.random.fold_in(keys[10], 1), 1, FFB).astype(jnp.int32)
    heads_on = place_ends(jax.random.randint(keys[11], (MICRO, LAYERS), 1, HEADS + 1), jax.random.fold_in(keys[11], 1), 1, HEADS).astype(jnp.int32)
    return {"hidden_in": hidden_in, "attn_gain": attn_gain, "w_query": w_query, "w_key": w_key, "w_value": w_value, "w_out": w_out, "ffn_gain": ffn_gain, "w_gate": w_gate, "w_up": w_up, "w_down": w_down, "ffn_blocks": ffn_blocks, "heads_on": heads_on}


ROPE_BASE = 500000.0
EPSILON = 1e-05

def rms_scale(values, gain_row):
    mean_sq = lax.optimization_barrier(jnp.mean(values * values, axis=-1, keepdims=True))
    return values * lax.rsqrt(mean_sq + EPSILON) * gain_row.astype(jnp.float32)

def rotate(values):
    length = values.shape[0]
    half_dim = values.shape[-1] // 2
    frequency = ROPE_BASE ** (-(jnp.arange(half_dim, dtype=jnp.float32) / half_dim))
    angles = jnp.arange(length, dtype=jnp.float32)[:, None] * frequency[None, :]
    cosine_table = jnp.cos(angles)[:, None, :]
    sine_table = jnp.sin(angles)[:, None, :]
    front_half = values[..., :half_dim].astype(jnp.float32)
    back_half = values[..., half_dim:].astype(jnp.float32)
    return jnp.concatenate([front_half * cosine_table - back_half * sine_table, front_half * sine_table + back_half * cosine_table], axis=-1)

def group_sum(left, right):
    length, inner = left.shape
    group_width = inner // N_MP
    left_groups = left.reshape(length, N_MP, group_width).astype(jnp.float32)
    right_groups = right.reshape(N_MP, group_width, right.shape[1]).astype(jnp.float32)
    partials = jnp.einsum('tgk,gkd->gtd', left_groups, right_groups).astype(jnp.bfloat16)
    return lax.optimization_barrier(jnp.sum(partials.astype(jnp.float32), axis=0))

def layer_step(carried, layer_pos, active, block_count, attn_gain, w_query, w_key, w_value, w_out, ffn_gain, w_gate, w_up, w_down):
    length = carried.shape[0]
    group_size = HEADS // KV_HEADS
    residual = carried.astype(jnp.float32)
    normed = rms_scale(residual, attn_gain[layer_pos]).astype(jnp.bfloat16)
    queries = rotate(jnp.dot(normed, w_query[layer_pos], preferred_element_type=jnp.float32).reshape(length, HEADS, HD)).astype(jnp.bfloat16)
    key_proj = jnp.dot(normed, w_key[layer_pos], preferred_element_type=jnp.float32).astype(jnp.bfloat16).reshape(length, HD, KV_HEADS).transpose(0, 2, 1)
    keys_rot = rotate(key_proj).astype(jnp.bfloat16)
    values = jnp.dot(normed, w_value[layer_pos], preferred_element_type=jnp.float32).astype(jnp.bfloat16).reshape(length, HD, KV_HEADS).transpose(0, 2, 1)
    keys_all = jnp.repeat(keys_rot, group_size, axis=1)
    values_all = jnp.repeat(values, group_size, axis=1)
    scores = jnp.einsum('qhd,khd->hqk', queries.astype(jnp.float32), keys_all.astype(jnp.float32)) * HD ** (-0.5)
    causal = jnp.arange(length)[:, None] >= jnp.arange(length)[None, :]
    scores = jnp.where(causal[None], scores, -jnp.inf)
    probabilities = jax.nn.softmax(scores, axis=-1).astype(jnp.bfloat16)
    context = jnp.einsum('hqk,khd->qhd', probabilities.astype(jnp.float32), values_all.astype(jnp.float32))
    head_ids = jnp.arange(HEADS)
    context = jnp.where((head_ids < active)[None, :, None], context, 0.0).astype(jnp.bfloat16)
    attended = residual + group_sum(context.reshape(length, HEADS * HD), w_out[layer_pos])
    normed_ffn = rms_scale(attended, ffn_gain[layer_pos]).astype(jnp.bfloat16)
    gate_part = jnp.dot(normed_ffn, w_gate[layer_pos][:, :FF], preferred_element_type=jnp.float32)
    up_part = jnp.dot(normed_ffn, w_up[layer_pos][:, :FF], preferred_element_type=jnp.float32)
    unit_ids = jnp.arange(FF)
    hidden = jnp.where((unit_ids < BLOCK * block_count)[None, :], jax.nn.silu(gate_part) * up_part, 0.0).astype(jnp.bfloat16)
    padded = jnp.pad(hidden, ((0, 0), (0, w_gate.shape[2] - FF)))
    return (attended + group_sum(padded, w_down[layer_pos])).astype(jnp.bfloat16)

def reference(hidden_in, attn_gain, w_query, w_key, w_value, w_out, ffn_gain, w_gate, w_up, w_down, ffn_blocks, heads_on):
    finished = []
    for micro_index in range(MICRO):
        carried = hidden_in[micro_index // SECTIONS, micro_index % SECTIONS]
        for layer_pos in range(LAYERS):
            carried = layer_step(carried, layer_pos, heads_on[micro_index, layer_pos], ffn_blocks[micro_index, layer_pos], attn_gain, w_query, w_key, w_value, w_out, ffn_gain, w_gate, w_up, w_down)
        finished.append(carried)
    return jnp.stack(finished).reshape(MICRO_DEV, SECTIONS, LEN, D)
```

```python
import jax
import jax.numpy as jnp
import numpy as np
from jax import lax
from jax.experimental import pallas as pl
from jax.experimental.pallas import tpu as pltpu
from jax.sharding import PartitionSpec as P

HEADS = 32
KV_HEADS = 8
HD = 128
BLOCK = 128


ROPE_BASE = 500000.0
EPSILON = 1e-05


def passed_along(array, axis, by):
    peers = lax.axis_size(axis)
    return lax.ppermute(array, axis, [(i, (i + by) % peers) for i in range(peers)])


def rms_scale(values, gain_row):
    mean_sq = jnp.mean(values * values, axis=-1, keepdims=True)
    return values * lax.rsqrt(mean_sq + EPSILON) * gain_row.astype(jnp.float32)


def rotate(values):
    length = values.shape[0]
    half_dim = values.shape[-1] // 2
    frequency = ROPE_BASE ** (-(jnp.arange(half_dim, dtype=jnp.float32) / half_dim))
    angles = jnp.arange(length, dtype=jnp.float32)[:, None] * frequency[None, :]
    cosine_table = jnp.cos(angles)[:, None, :]
    sine_table = jnp.sin(angles)[:, None, :]
    front_half = values[..., :half_dim].astype(jnp.float32)
    back_half = values[..., half_dim:].astype(jnp.float32)
    return jnp.concatenate(
        [
            front_half * cosine_table - back_half * sine_table,
            front_half * sine_table + back_half * cosine_table,
        ],
        axis=-1,
    )


def attend_local(projected, query_width, key_width, active, first_head):
    length = projected.shape[0]
    heads_here = query_width // HD
    group_size = HEADS // KV_HEADS
    queries = rotate(projected[:, :query_width].reshape(length, heads_here, HD)).astype(
        jnp.bfloat16
    )
    key_local = projected[:, query_width : query_width + key_width].astype(jnp.bfloat16)
    value_local = projected[:, query_width + key_width :].astype(jnp.bfloat16)
    key_whole, value_whole = (
        lax.all_gather(key_local, "mp", axis=1, tiled=True),
        lax.all_gather(value_local, "mp", axis=1, tiled=True),
    )
    key_heads = key_whole.reshape(length, HD, KV_HEADS).transpose(0, 2, 1)
    value_heads = value_whole.reshape(length, HD, KV_HEADS).transpose(0, 2, 1)
    kv_here = max(1, heads_here // group_size)
    repeat_count = heads_here // kv_here
    first_kv = first_head // group_size
    key_pick = lax.dynamic_slice_in_dim(key_heads, first_kv, kv_here, 1)
    value_pick = lax.dynamic_slice_in_dim(value_heads, first_kv, kv_here, 1)
    keys_rot = jnp.repeat(rotate(key_pick).astype(jnp.bfloat16), repeat_count, axis=1)
    values = jnp.repeat(value_pick, repeat_count, axis=1)
    scores = jnp.einsum(
        "qhd,khd->hqk", queries, keys_rot, preferred_element_type=jnp.float32
    ) * HD ** (-0.5)
    causal = jnp.arange(length)[:, None] >= jnp.arange(length)[None, :]
    scores = jnp.where(causal[None], scores, -jnp.inf)
    probabilities = jax.nn.softmax(scores, axis=-1).astype(jnp.bfloat16)
    context = jnp.einsum("hqk,khd->qhd", probabilities, values, preferred_element_type=jnp.float32)
    head_ids = first_head + jnp.arange(heads_here)
    context = jnp.where((head_ids < active)[None, :, None], context, 0.0).astype(jnp.bfloat16)
    return context.reshape(length, query_width)


def per_device(
    hidden_in,
    attn_gain,
    w_query,
    w_key,
    w_value,
    w_out,
    ffn_gain,
    w_gate,
    w_up,
    w_down,
    ffn_blocks,
    heads_on,
):
    section_count = lax.axis_size("section")
    section_index = lax.axis_index("section")
    model_count = lax.axis_size("mp")
    model_index = lax.axis_index("mp")
    micro_total = ffn_blocks.shape[0]
    per_section = hidden_in.shape[0]
    length = hidden_in.shape[2]
    model_width = hidden_in.shape[3]
    local_rows = length // model_count
    units_here = w_gate.shape[2]
    query_width = w_query.shape[2]
    key_width = w_key.shape[2]
    first_head = model_index * (query_width // HD)
    first_unit = model_index * units_here
    joined_qkv = [jnp.concatenate([w_query[0], w_key[0], w_value[0]], axis=1)]
    joined_pair = [jnp.concatenate([w_gate[0], w_up[0]], axis=1)]

    def gated(pre_act, block_count):
        gate_part = pre_act[:, :units_here]
        up_part = pre_act[:, units_here:]
        unit_ids = first_unit + jnp.arange(units_here)
        return jnp.where(
            (unit_ids < BLOCK * block_count)[None, :], jax.nn.silu(gate_part) * up_part, 0.0
        ).astype(jnp.bfloat16)

    def layer_rows(carried, layer_pos, active, block_count):
        residual = carried.astype(jnp.float32)
        normed = rms_scale(residual, attn_gain[layer_pos]).astype(jnp.bfloat16)
        projected = jnp.dot(
            lax.all_gather(normed, "mp", axis=0, tiled=True),
            joined_qkv[layer_pos],
            preferred_element_type=jnp.float32,
        )
        context = attend_local(projected, query_width, key_width, active, first_head)
        attended = residual + lax.psum_scatter(
            jnp.dot(context, w_out[layer_pos], preferred_element_type=jnp.float32).astype(
                jnp.bfloat16
            ),
            "mp",
            scatter_dimension=0,
            tiled=True,
        ).astype(jnp.float32)
        normed_ffn = rms_scale(attended, ffn_gain[layer_pos]).astype(jnp.bfloat16)
        hidden = gated(
            jnp.dot(
                lax.all_gather(normed_ffn, "mp", axis=0, tiled=True),
                joined_pair[layer_pos],
                preferred_element_type=jnp.float32,
            ),
            block_count,
        )
        return (
            attended
            + lax.psum_scatter(
                jnp.dot(hidden, w_down[layer_pos], preferred_element_type=jnp.float32).astype(
                    jnp.bfloat16
                ),
                "mp",
                scatter_dimension=0,
                tiled=True,
            ).astype(jnp.float32)
        ).astype(jnp.bfloat16)

    def section_work(carried, moment, layer_fn):
        micro_index = jnp.clip(moment - section_index, 0, micro_total - 1)
        carried = layer_fn(carried, 0, heads_on[micro_index, 0], ffn_blocks[micro_index, 0])
        return carried

    def tick_step(moment, loop_carry):
        carried, slot_buffer = loop_carry
        cycle_index = moment // section_count
        incoming = lax.dynamic_index_in_dim(
            slot_buffer, jnp.minimum(cycle_index, per_section - 1), 0, keepdims=False
        )
        incoming = jnp.where(moment < micro_total, incoming, jnp.zeros_like(incoming))
        at_head = section_index == 0
        written = lax.dynamic_update_index_in_dim(
            slot_buffer, carried, jnp.maximum(cycle_index - 1, 0), 0
        )
        slot_buffer = jnp.where(at_head & (moment >= section_count), written, slot_buffer)
        carried = jnp.where(at_head, incoming, carried)
        carried = section_work(carried, moment, layer_rows)
        carried = passed_along(carried, "section", 1)
        slot_buffer = passed_along(slot_buffer, "section", -1)
        return (carried, slot_buffer)

    slot_start = hidden_in.reshape(per_section, length, model_width)
    slot_start = lax.dynamic_slice_in_dim(slot_start, model_index * local_rows, local_rows, 1)
    initial = jnp.zeros((local_rows, model_width), jnp.bfloat16)
    finished = lax.fori_loop(0, micro_total + section_count, tick_step, (initial, slot_start))
    result = finished[1]
    result = lax.all_gather(result, "mp", axis=1, tiled=True)
    return result.reshape(hidden_in.shape)


MESH = pl.DeviceIdType.MESH
BF16 = jnp.bfloat16
F32 = jnp.float32
TILE = 256
WIDE = 512


def tables(length):
    half = HD // 2
    frequency = np.float32(ROPE_BASE) ** (-(np.arange(half, dtype=np.float32) / np.float32(half)))
    angles = np.arange(length, dtype=np.float32)[:, None] * frequency[None, :].astype(np.float32)
    cosine, sine = np.cos(angles), np.sin(angles)
    q_cos = np.concatenate([cosine, cosine], axis=1)
    q_sin = np.concatenate([-sine, sine], axis=1)
    k_cos = np.concatenate([q_cos.T, np.ones((HD, length))], axis=1)
    k_sin = np.concatenate([q_sin.T, np.zeros((HD, length))], axis=1)
    return [jnp.asarray(t, F32) for t in (q_cos, q_sin, k_cos, k_sin)]


def remote(src, dst, send_sem, recv_sem, where):
    return pltpu.make_async_remote_copy(
        src_ref=src,
        dst_ref=dst,
        send_sem=send_sem,
        recv_sem=recv_sem,
        device_id=where,
        device_id_type=MESH,
    )


def layer_kernel(
    sections,
    peers,
    heads_on,
    ffn_blocks,
    hidden_in,
    attn_gain,
    ffn_gain,
    q_cos,
    q_sin,
    k_cos,
    k_sin,
    w_query,
    w_key,
    w_value,
    w_out,
    w_gate,
    w_up,
    w_down,
    out,
    v_query,
    v_kv,
    v_out,
    v_gate,
    v_up,
    v_down,
    inbox,
    outbox,
    home,
    rows_f32,
    gathered,
    normed,
    kv_send,
    kv_recv,
    context,
    hidden,
    part,
    pair_in,
    chip_send,
    chip_in,
    weight_sem,
    inbox_sem,
    outbox_sem,
    seed_sem,
    home_sem,
    gather_send,
    gather_recv,
    relay_send,
    relay_recv,
    kv_send_sem,
    kv_recv_sem,
    pair_sem,
    chip_send_sem,
    chip_recv_sem,
    out_sem,
):
    sec = lax.axis_index("section")
    me = lax.axis_index("mp")
    chips = peers // 2
    chip, core = me // 2, me % 2
    slot = core * chips + chip
    mate = (sec, chip * 2 + 1 - core)
    last = sections - 1
    rows, width = rows_f32.shape
    length = peers * rows
    heads_here = v_query.shape[1] // HD
    key_width = w_key.shape[1]
    units = v_gate.shape[1]

    def chip_at(step):
        other = (chip + step) % chips
        return other, (sec, other * 2 + core)

    def weight_copies():
        pairs = (
            (w_query, v_query),
            (w_key, v_kv.at[:, pl.ds(0, key_width)]),
            (w_value, v_kv.at[:, pl.ds(key_width, key_width)]),
            (w_out, v_out),
            (w_gate, v_gate),
            (w_up, v_up),
            (w_down, v_down),
        )
        return [
            pltpu.make_async_copy(a, b, weight_sem.at[i]) for i, (a, b) in enumerate(pairs)
        ]

    seed = pltpu.make_async_copy(hidden_in.at[slot], home, seed_sem)
    seed.start()
    for copy in weight_copies():
        copy.start()

    barrier = pltpu.get_barrier_semaphore()
    for step in range(1, peers):
        pl.semaphore_signal(barrier, inc=1, device_id=(sec, (me + step) % peers), device_id_type=MESH)
    for step in range(1, sections):
        pl.semaphore_signal(barrier, inc=1, device_id=((sec + step) % sections, me), device_id_type=MESH)
    pl.semaphore_wait(barrier, peers + sections - 2)

    seed.wait()
    own = remote(home, inbox.at[sec], outbox_sem.at[0], inbox_sem.at[sec], (0, me))

    @pl.when(sec == 0)
    def _():
        inbox[0] = home[...]

    @pl.when(sec != 0)
    def _():
        own.start()
        own.wait_send()

    def all_gather():
        mine = gathered.at[slot]
        to_mate = remote(mine, mine, gather_send.at[chips - 1], gather_recv.at[chips - 1], mate)
        sends = []
        for k in (list(range(1, chips, 2)) + list(range(2, chips, 2))):
            _, where = chip_at(k)
            sends.append(remote(mine, mine, gather_send.at[k - 1], gather_recv.at[k - 1], where))
            sends[-1].start()
        to_mate.start()
        relays = []
        for k in (list(range(1, chips, 2)) + list(range(2, chips, 2))):
            other, where = chip_at(chips - k)
            block = gathered.at[core * chips + other]
            remote(block, block, gather_send.at[k - 1], gather_recv.at[k - 1], where).wait_recv()
            relays.append(remote(block, block, relay_send.at[k - 1], relay_recv.at[k - 1], mate))
            relays[-1].start()
        to_mate.wait_recv()
        for k in range(1, chips):
            other, _ = chip_at(chips - k)
            block = gathered.at[(1 - core) * chips + other]
            remote(block, block, relay_send.at[k - 1], relay_recv.at[k - 1], mate).wait_recv()
        for copy in sends + relays + [to_mate]:
            copy.wait_send()

    def widen():
        columns = width // 4
        for i in range(4):
            at = pl.ds(i * columns, columns)
            block = gathered[:, :, at].astype(F32)
            normed[:, at] = block.reshape(length, columns).astype(BF16)

    def norm_rows(gain):
        x = rows_f32[...]
        scale = lax.rsqrt(jnp.mean(x * x, axis=-1, keepdims=True) + EPSILON)
        gathered[slot] = (x * scale * gain[...].astype(F32)).astype(BF16)

    def reduce_rows():
        other_half = part.at[pl.ds((1 - core) * chips, chips)]
        across = remote(other_half, pair_in, pair_sem.at[0], pair_sem.at[1], mate)
        across.start()
        across.wait_recv()
        for k in range(1, chips):
            other, where = chip_at(k)
            both = part[core * chips + other].astype(F32) + pair_in[other].astype(F32)
            chip_send[k - 1] = both.astype(BF16)
            remote(
                chip_send.at[k - 1], chip_in.at[k - 1], chip_send_sem.at[k - 1], chip_recv_sem.at[k - 1], where
            ).start()
        rows_f32[...] = rows_f32[...] + (part[slot].astype(F32) + pair_in[chip].astype(F32))
        for k in range(1, chips):
            _, where = chip_at(k)
            remote(
                chip_send.at[k - 1], chip_in.at[k - 1], chip_send_sem.at[k - 1], chip_recv_sem.at[k - 1], where
            ).wait()
            rows_f32[...] = rows_f32[...] + chip_in[k - 1].astype(F32)
        across.wait_send()

    def project_rows(left, weight):
        def step(i, _):
            at = pl.ds(pl.multiple_of(i * WIDE, WIDE), WIDE)
            term = jnp.dot(left[...], weight[:, at], preferred_element_type=F32)
            part[:, :, at] = term.reshape(peers, rows, WIDE).astype(BF16)
            return 0

        lax.fori_loop(0, width // WIDE, step, 0)

    def exchange_kv():
        copies = []
        for step in range(1, peers):
            to = (me + step) % peers
            copies.append(
                remote(
                    kv_send.at[to], kv_recv.at[me], kv_send_sem.at[step - 1], kv_recv_sem.at[step - 1], (sec, to)
                )
            )
            copies[-1].start()
        kv_recv[me] = kv_send[me]
        return copies

    def attention(active):
        left = normed[...]
        kv = jnp.dot(left, v_kv[...], preferred_element_type=F32).astype(BF16)
        stacked = jnp.concatenate([kv[:, :key_width], kv[:, key_width:]], axis=0)
        r = lax.broadcasted_iota(jnp.int32, (key_width, key_width), 0)
        c = lax.broadcasted_iota(jnp.int32, (key_width, key_width), 1)
        parts_here = key_width // KV_HEADS
        pick = jnp.where(c == (r % parts_here) * KV_HEADS + r // parts_here, 1.0, 0.0).astype(BF16)
        by_head = lax.dot_general(
            pick, stacked, (((1,), (1,)), ((), ())), preferred_element_type=F32
        )
        kv_send[...] = by_head.astype(BF16).reshape(KV_HEADS, parts_here, 2 * length)
        copies = exchange_kv()
        query = jnp.dot(left, v_query[...], preferred_element_type=F32)
        heads = []
        for h in range(heads_here):
            head = query[:, h * HD : (h + 1) * HD]
            heads.append(
                (head * q_cos[...] + pltpu.roll(head, HD // 2, 1) * q_sin[...]).astype(BF16)
            )
        queries = jnp.concatenate(heads, axis=0)
        for copy in copies:
            copy.wait()
        pair = kv_recv[...].reshape(HD, 2 * length).astype(F32)
        swapped = jnp.concatenate([pair[HD // 2 :], pair[: HD // 2]], axis=0)
        pair = (pair * k_cos[...] + swapped * k_sin[...]).astype(BF16)
        scores = jnp.dot(queries, pair, preferred_element_type=F32) * HD ** (-0.5)
        token = lax.broadcasted_iota(jnp.int32, scores.shape, 0) % length
        key_at = lax.broadcasted_iota(jnp.int32, scores.shape, 1)
        scores = jnp.where(key_at <= token, scores, -jnp.inf)
        scores = jnp.exp(scores - jnp.max(scores, axis=-1, keepdims=True))
        chances = scores / jnp.sum(scores, axis=-1, keepdims=True)
        chances = pltpu.roll(chances, length, 1).astype(BF16)
        mixed = lax.dot_general(
            chances, pair, (((1,), (1,)), ((), ())), preferred_element_type=F32
        )
        for h in range(heads_here):
            on = me * heads_here + h < active
            block = mixed[h * length : (h + 1) * length]
            context[:, h * HD : (h + 1) * HD] = jnp.where(on, block, 0.0).astype(BF16)

    def feed_forward(block_count):
        def step(i, _):
            at = pl.ds(pl.multiple_of(i * TILE, TILE), TILE)
            left = normed[...]
            gate = jnp.dot(left, v_gate[:, at], preferred_element_type=F32)
            up = jnp.dot(left, v_up[:, at], preferred_element_type=F32)
            unit = me * units + i * TILE + lax.broadcasted_iota(jnp.int32, gate.shape, 1)
            value = gate / (1.0 + jnp.exp(-gate)) * up
            hidden[:, at] = jnp.where(unit < BLOCK * block_count, value, 0.0).astype(BF16)
            return 0

        lax.fori_loop(0, units // TILE, step, 0)

    def micro_step(m, _):
        arrived = remote(home, inbox.at[m], outbox_sem.at[0], inbox_sem.at[m], (0, me))

        @pl.when((sec != 0) | (m != 0))
        def _():
            arrived.wait_recv()

        rows_f32[...] = inbox[m].astype(F32)
        norm_rows(attn_gain)
        all_gather()
        widen()

        def when_loaded(first, stop):
            @pl.when(m == 0)
            def _():
                for copy in weight_copies()[first:stop]:
                    copy.wait()

        when_loaded(0, 3)
        attention(heads_on[m, 0])
        when_loaded(3, 4)
        project_rows(context, v_out)
        reduce_rows()
        norm_rows(ffn_gain)
        all_gather()
        widen()
        when_loaded(4, 6)
        feed_forward(ffn_blocks[m, 0])
        when_loaded(6, 7)
        project_rows(hidden, v_down)
        reduce_rows()
        outbox[m] = rows_f32[...].astype(BF16)

        @pl.when(sec < last)
        def _():
            remote(outbox.at[m], inbox.at[m], outbox_sem.at[m], inbox_sem.at[m], (sec + 1, me)).start()

        @pl.when((sec == last) & (m < last))
        def _():
            remote(outbox.at[m], home, outbox_sem.at[m], home_sem, (m, me)).start()

        return 0

    lax.fori_loop(0, sections, micro_step, 0)

    for m in range(sections):
        sent = remote(outbox.at[m], home, outbox_sem.at[m], home_sem, (0, me))
        if m < last:
            sent.wait_send()
        else:

            @pl.when(sec < last)
            def _():
                sent.wait_send()

    @pl.when(sec < last)
    def _():
        remote(outbox.at[0], home, outbox_sem.at[0], home_sem, (last, me)).wait_recv()
        gathered[slot] = home[...]

    @pl.when(sec == last)
    def _():
        gathered[slot] = outbox[last]

    all_gather()
    done = pltpu.make_async_copy(gathered, out, out_sem)
    done.start()
    done.wait()


def resident(hidden_in, attn_gain, w_query, w_key, w_value, w_out, ffn_gain, w_gate, w_up, w_down, ffn_blocks, heads_on):
    sections, peers = lax.axis_size("section"), lax.axis_size("mp")
    length, width = hidden_in.shape[2:]
    rows, chips = length // peers, peers // 2
    units, key_width = w_gate.shape[2], w_key.shape[2]
    query_width = w_query.shape[2]
    parts_here = key_width // KV_HEADS
    smem = pl.BlockSpec(memory_space=pltpu.SMEM)
    vmem = pl.BlockSpec(memory_space=pltpu.VMEM)
    hbm = pl.BlockSpec(memory_space=pl.ANY)
    dma = pltpu.SemaphoreType.DMA
    half = pltpu.VMEM
    result = pl.pallas_call(
        lambda *refs: layer_kernel(sections, peers, *refs),
        out_shape=jax.ShapeDtypeStruct((peers, rows, width), BF16),
        in_specs=[smem, smem, hbm] + [vmem] * 6 + [hbm] * 7,
        out_specs=hbm,
        scratch_shapes=[
            half((width, query_width), BF16),
            half((width, 2 * key_width), BF16),
            half((query_width, width), BF16),
            half((width, units), BF16),
            half((width, units), BF16),
            half((units, width), BF16),
            half((sections, rows, width), BF16),
            half((sections, rows, width), BF16),
            half((rows, width), BF16),
            half((rows, width), F32),
            half((peers, rows, width), BF16),
            half((length, width), BF16),
            half((peers, parts_here, 2 * length), BF16),
            half((peers, parts_here, 2 * length), BF16),
            half((length, query_width), BF16),
            half((length, units), BF16),
            half((peers, rows, width), BF16),
            half((chips, rows, width), BF16),
            half((chips - 1, rows, width), BF16),
            half((chips - 1, rows, width), BF16),
            dma((7,)),
            dma((sections,)),
            dma((sections,)),
            dma,
            dma,
            dma((chips,)),
            dma((chips,)),
            dma((chips - 1,)),
            dma((chips - 1,)),
            dma((peers - 1,)),
            dma((peers - 1,)),
            dma((2,)),
            dma((chips - 1,)),
            dma((chips - 1,)),
            dma,
        ],
        compiler_params=pltpu.CompilerParams(
            collective_id=0, has_side_effects=True, vmem_limit_bytes=67043328
        ),
    )(
        heads_on,
        ffn_blocks,
        hidden_in.reshape(peers, rows, width),
        attn_gain,
        ffn_gain,
        *tables(length),
        w_query[0],
        w_key[0],
        w_value[0],
        w_out[0],
        w_gate[0],
        w_up[0],
        w_down[0],
    )
    return result.reshape(hidden_in.shape)


def one_device(*args):
    hidden_in, w_query, w_key, w_gate = args[0], args[2], args[3], args[7]
    sections, peers = lax.axis_size("section"), lax.axis_size("mp")
    fits = (
        hidden_in.shape[0] == 1
        and args[10].shape[0] == sections
        and peers == KV_HEADS
        and hidden_in.shape[2] == 8 * peers
        and 2 * hidden_in.shape[2] == HD
        and w_query.shape[2] * KV_HEADS == HEADS * HD
        and w_key.shape[2] == HD
        and w_gate.shape[2] % TILE == 0
        and hidden_in.shape[3] % WIDE == 0
    )
    return (resident if fits else per_device)(*args)


def solution(mesh):
    return jax.shard_map(
        one_device,
        mesh=mesh,
        in_specs=(
            P(None, "section", None, None),
            P("section", None),
            P("section", None, "mp"),
            P("section", None, "mp"),
            P("section", None, "mp"),
            P("section", "mp", None),
            P("section", None),
            P("section", None, "mp"),
            P("section", None, "mp"),
            P("section", "mp", None),
            P(None, "section"),
            P(None, "section"),
        ),
        out_specs=P(None, "section", None, None),
        check_vma=False,
    )
```
